32 devices in a mesh: fsdp: 16 (over z, y, core), tp: 2 (over x).
Axes of the slice: x: 2, y: 2, z: 4, core: 2. Of those that a mesh axis runs over, the one named last changes fastest.
Arguments:
- hidden: bfloat16 [32, 5120], P(None, 'fsdp'), may hold values from -20 to 20
- query_weight: bfloat16 [5120, 5120], P(None, ('tp', 'fsdp')), may hold values from -0.078125 to 0.078125
- key_weight: bfloat16 [5120, 1024], P(None, ('tp', 'fsdp')), may hold values from -0.078125 to 0.078125
- value_weight: bfloat16 [5120, 1024], P(None, ('tp', 'fsdp')), may hold values from -0.078125 to 0.078125
- output_weight: bfloat16 [5120, 5120], P(('tp', 'fsdp')), may hold values from -0.078125 to 0.078125
- gate_weight: bfloat16 [5120, 27648], P(None, ('tp', 'fsdp')), may hold values from -0.078125 to 0.078125
- up_weight: bfloat16 [5120, 27648], P(None, ('tp', 'fsdp')), may hold values from -0.078125 to 0.078125
- down_weight: bfloat16 [27648, 5120], P(('tp', 'fsdp')), may hold values from -0.0390625 to 0.0390625
- history: float32 [7, 1024], replicated, may hold values from 0.0001 to 1, as said below
- slot: int32 [1], replicated, may hold values from 0 to 1023
- lengths: int32 [32], P('fsdp'), may hold values from 512 to 4096, as said below
- key_cache: bfloat16 [32, 4096, 1024], P('fsdp', None, 'tp'), may hold values from -1000 to 1000
- value_cache: bfloat16 [32, 4096, 1024], P('fsdp', None, 'tp'), may hold values from -6 to 6
Outputs:
- attention_out: bfloat16 [32, 5120], P('fsdp', 'tp')
- query_rollout: bfloat16 [5120, 5120], P('fsdp', 'tp')
- key_rollout: bfloat16 [5120, 1024], P('fsdp', 'tp')
- value_rollout: bfloat16 [5120, 1024], P('fsdp', 'tp')
- output_rollout: bfloat16 [5120, 5120], P('tp', 'fsdp')
- gate_rollout: bfloat16 [5120, 27648], P('fsdp', 'tp')
- up_rollout: bfloat16 [5120, 27648], P('fsdp', 'tp')
- down_rollout: bfloat16 [27648, 5120], P('tp', 'fsdp')
- new_history: float32 [7, 1024], replicated
The draws below stay inside these ranges and needn't reach their ends.
Inputs may be any that keep to these rules, and one draw needn't show every extreme that they name: `history`: strictly positive. `lengths`: some sequence has all 4096 slots valid.
All inputs are finite; a program needn't handle non-finite values.
Results may differ from the reference program's by a relative error of at most 0.012.
The reference program's roundings to bfloat16 on the way (of `probs`) count: a program that leaves them out, or rounds other values in their place, can miss the bound.
Values may be sent and summed in bfloat16 or wider, within the bound.
A program may use at most 192 MiB of HBM per device.

```python
import jax
import jax.numpy as jnp
from jax import lax

D = 5120
F = 27648
HEADS = 40
KV_HEADS = 8
HEAD_DIM = 128
HIST = 1024
CACHE = 4096
SEQS = 32


def draw_hidden(key, part):
    values = jnp.clip(jax.random.normal(jax.random.fold_in(key, 11), (SEQS, D), jnp.float32), -6.0, 6.0)
    return values.astype(jnp.bfloat16)


def draw_history(key, part):
    fans = jnp.array([D, D, D, D, D, D, F], jnp.float32)
    low, high = (3.0, 12.0)
    levels = jnp.exp(jax.random.uniform(jax.random.fold_in(key, 21), (7,), jnp.float32, jnp.log(low), jnp.log(high)))
    spread = jnp.exp(jax.random.uniform(jax.random.fold_in(key, 22), (7, HIST), jnp.float32, jnp.log(0.02), 0.0))
    return (fans ** (-0.5) * levels)[:, None] * spread


def draw_lengths(key, part):
    counts = jax.random.randint(jax.random.fold_in(key, 31), (SEQS,), CACHE // 8, CACHE + 1)
    chosen = jax.random.randint(jax.random.fold_in(key, 32), (), 0, SEQS)
    return jnp.where(jnp.arange(SEQS) == chosen, CACHE, counts).astype(jnp.int32)


def draw_key_cache(key, part):
    values = jnp.clip(jax.random.normal(jax.random.fold_in(key, 41), (SEQS, CACHE, KV_HEADS * HEAD_DIM), jnp.float32), -6.0, 6.0)
    return values.astype(jnp.bfloat16)


def block_scale(own_key, shape, cuts, low, top_value):
    level, own = 1.0, jax.random.fold_in(own_key, 6)
    for dim, shards_of in cuts:
        heights = jnp.exp(jax.random.uniform(jax.random.fold_in(own, dim), (shards_of,), jnp.float32, low / len(cuts), top_value / len(cuts)))
        level = level * jnp.repeat(heights, shape[dim] // shards_of).reshape([-1 if axis == dim else 1 for axis in range(len(shape))])
    return level


def scatter_about(rng, extent, width, reach, cuts=(), kind=jnp.bfloat16):
    loudness = block_scale(rng, extent, cuts, -0.22, 0.18) if cuts else 1.0
    values = jax.random.normal(rng, extent, jnp.float32) * width * loudness
    return jnp.minimum(jnp.maximum(values, -reach), reach).astype(kind)


def setup_inputs(seed: int = 0) -> dict:
    streams_of = jax.random.split(jax.random.key(seed), 14)
    hidden = draw_hidden(jax.random.fold_in(streams_of[13], 71), 0)
    query_weight = scatter_about(streams_of[1], (D, D), D ** -0.5, 0.078125, ((1, 32),))
    key_weight = scatter_about(streams_of[2], (D, KV_HEADS * HEAD_DIM), D ** -0.5, 0.078125, ((1, 32),))
    value_weight = scatter_about(streams_of[3], (D, KV_HEADS * HEAD_DIM), D ** -0.5, 0.078125, ((1, 32),))
    output_weight = scatter_about(streams_of[4], (D, D), D ** -0.5, 0.078125, ((0, 32),))
    gate_weight = scatter_about(streams_of[5], (D, F), D ** -0.5, 0.078125, ((1, 32),))
    up_weight = scatter_about(streams_of[6], (D, F), D ** -0.5, 0.078125, ((1, 32),))
    down_weight = scatter_about(streams_of[7], (F, D), F ** -0.5, 0.0390625, ((0, 32),))
    history = draw_history(jax.random.fold_in(streams_of[13], 71), 0)
    slot = jax.random.randint(streams_of[9], (1,), 0, HIST).astype(jnp.int32)
    lengths = draw_lengths(jax.random.fold_in(streams_of[13], 71), 0)
    key_cache = draw_key_cache(jax.random.fold_in(streams_of[13], 71), 0)
    value_cache = scatter_about(streams_of[12], (SEQS, CACHE, KV_HEADS * HEAD_DIM), 1.0, 6.0, ((0, 16), (2, 2)))
    return dict(hidden=hidden, query_weight=query_weight, key_weight=key_weight, value_weight=value_weight, output_weight=output_weight, gate_weight=gate_weight, up_weight=up_weight, down_weight=down_weight, history=history, slot=slot, lengths=lengths, key_cache=key_cache, value_cache=value_cache)


target_peak = 4.0
norm_eps = 1e-06
rope_theta = 1000000.0

def largest(tensor):
    return jnp.max(jnp.abs(tensor.astype(jnp.float32)))

def scaling(peaks, history, slot):
    marked = lax.broadcasted_iota(jnp.int32, history.shape, 1) == slot[0]
    kept = lax.optimization_barrier(jnp.max(jnp.where(marked, jnp.zeros_like(history), history), axis=1))
    return (target_peak / jnp.maximum(peaks, kept), jnp.where(marked, peaks[:, None], history))

def quantize(tensor, factor):
    return (tensor.astype(jnp.float32) * factor).astype(jnp.bfloat16)

def rotate(vectors, positions):
    half_dim = vectors.shape[-1] // 2
    ladder = jnp.arange(half_dim, dtype=jnp.float32)
    spread = rope_theta ** (-2.0 * ladder / vectors.shape[-1])
    angle = positions.astype(jnp.float32)[:, None] * spread[None, :]
    cosine = jnp.cos(angle)[:, None, :]
    sine = jnp.sin(angle)[:, None, :]
    first = vectors[..., :half_dim]
    second = vectors[..., half_dim:]
    return jnp.concatenate([first * cosine - second * sine, second * cosine + first * sine], axis=-1)

def one_sequence(items):
    query, key_new, value_new, cached_keys, cached_values, length = items
    kv_count = query.shape[0]
    head_dim = query.shape[2]
    cache_len = cached_keys.shape[0]
    keys = cached_keys.reshape(cache_len, kv_count, head_dim).astype(jnp.float32)
    values = cached_values.reshape(cache_len, kv_count, head_dim).astype(jnp.float32)
    scale = head_dim ** (-0.5)
    widened = query.astype(jnp.float32)
    scores = jnp.einsum('kgd,jkd->kgj', widened, keys) * scale
    own = lax.optimization_barrier(jnp.sum(widened * key_new.astype(jnp.float32)[:, None, :], axis=-1)) * scale
    valid = (lax.broadcasted_iota(jnp.int32, (cache_len,), 0) < length)[None, None, :]
    top = jnp.maximum(lax.optimization_barrier(jnp.max(jnp.where(valid, scores, -1e+30), axis=-1)), own)
    weights = jnp.where(valid, jnp.exp(scores - top[..., None]), 0.0)
    own_weight = jnp.exp(own - top)
    total = lax.optimization_barrier(jnp.sum(weights, axis=-1)) + own_weight
    probs = (weights / total[..., None]).astype(jnp.bfloat16)
    own_prob = (own_weight / total).astype(jnp.bfloat16)
    mixed = jnp.einsum('kgj,jkd->kgd', probs.astype(jnp.float32), values)
    mixed = mixed + own_prob.astype(jnp.float32)[..., None] * value_new.astype(jnp.float32)[:, None, :]
    return mixed.astype(jnp.bfloat16).reshape(-1)

def reference(hidden, query_weight, key_weight, value_weight, output_weight, gate_weight, up_weight, down_weight, history, slot, lengths, key_cache, value_cache):
    trainer = [query_weight, key_weight, value_weight, output_weight, gate_weight, up_weight, down_weight]
    peaks = jnp.stack([largest(tensor) for tensor in trainer])
    factors, new_history = scaling(peaks, history, slot)
    rollout = [quantize(trainer[number], factors[number]) for number in range(7)]
    widened = hidden.astype(jnp.float32)
    inv_rms = lax.rsqrt(lax.optimization_barrier(jnp.mean(widened * widened, axis=1)) + norm_eps)[:, None]
    query = jnp.dot(hidden, rollout[0], preferred_element_type=jnp.float32) * inv_rms / factors[0]
    key_new = jnp.dot(hidden, rollout[1], preferred_element_type=jnp.float32) * inv_rms / factors[1]
    value_new = jnp.dot(hidden, rollout[2], preferred_element_type=jnp.float32) * inv_rms / factors[2]
    count_seq = hidden.shape[0]
    query = rotate(query.reshape(count_seq, HEADS, HEAD_DIM), lengths).astype(jnp.bfloat16)
    query = query.reshape(count_seq, KV_HEADS, HEADS // KV_HEADS, HEAD_DIM)
    key_new = rotate(key_new.reshape(count_seq, KV_HEADS, HEAD_DIM), lengths).astype(jnp.bfloat16)
    value_new = value_new.reshape(count_seq, KV_HEADS, HEAD_DIM).astype(jnp.bfloat16)
    attention_out = lax.map(one_sequence, (query, key_new, value_new, key_cache, value_cache, lengths))
    return (attention_out, rollout[0], rollout[1], rollout[2], rollout[3], rollout[4], rollout[5], rollout[6], new_history)
```

```python
import functools
import math

import jax
import jax.numpy as jnp
from jax import lax
from jax.experimental import pallas as pl
from jax.experimental.pallas import tpu as pltpu
from jax.sharding import PartitionSpec as P

HEAD_DIM = 128
LANES = 128
SLAB = 16


target_peak = 4.0
norm_eps = 1e-06
rope_theta = 1000000.0


def largest(tensor):
    return jnp.max(jnp.abs(tensor.astype(jnp.float32)))


def scaling(peaks, history, slot):
    marked = lax.broadcasted_iota(jnp.int32, history.shape, 1) == slot[0]
    kept = jnp.max(jnp.where(marked, jnp.zeros_like(history), history), axis=1)
    return (target_peak / jnp.maximum(peaks, kept), jnp.where(marked, peaks[:, None], history))


def quantize(tensor, factor):
    return (tensor.astype(jnp.float32) * factor).astype(jnp.bfloat16)


def rotate(vectors, positions):
    half_dim = vectors.shape[-1] // 2
    ladder = jnp.arange(half_dim, dtype=jnp.float32)
    spread = rope_theta ** (-2.0 * ladder / vectors.shape[-1])
    angle = positions.astype(jnp.float32)[:, None] * spread[None, :]
    cosine = jnp.cos(angle)[:, None, :]
    sine = jnp.sin(angle)[:, None, :]
    first = vectors[..., :half_dim]
    second = vectors[..., half_dim:]
    return jnp.concatenate(
        [first * cosine - second * sine, second * cosine + first * sine], axis=-1
    )


def after(tensor, *earlier):
    return lax.optimization_barrier((tensor,) + earlier)[0]


def exchange(blocks, *earlier):
    return lax.all_to_all(
        after(blocks, *earlier), "fsdp", split_axis=0, concat_axis=0, tiled=True
    )


def folds(width):
    rest = width % LANES
    return 1 if rest == 0 else LANES // math.gcd(rest, LANES)


def tile_rows(rows, width):
    return rows * width // LANES


def lane_index(rows):
    return lax.broadcasted_iota(jnp.int32, (rows, LANES), 1)


def assemble(pieces):
    total = sum(length for _, _, length in pieces)
    lanes = lane_index(pieces[0][0].shape[0])
    tiles = [None] * (total // LANES)
    offset = 0
    for value, start, length in pieces:
        shift = (offset - start) % LANES
        moved = pltpu.roll(value, shift, 1) if shift else value
        for tile in range(offset // LANES, (offset + length - 1) // LANES + 1):
            low = max(offset - tile * LANES, 0)
            old = tiles[tile]
            tiles[tile] = moved if low == 0 else jnp.where(lanes >= low, moved, old)
        offset += length
    return tiles


def cost(count):
    return pl.CostEstimate(flops=count, bytes_accessed=4 * count, transcendentals=0)


def columns_fit(count, rows, width):
    fold = folds(width)
    return rows % (SLAB * fold) == 0 and count % folds(width) == 0 and width >= 1


def rows_fit(count, rows, width):
    return count % 2 == 0 and width > LANES and width % LANES == LANES // 2 and rows % (2 * SLAB) == 0


def pack_columns_kernel(widths, rows, extra, *refs):
    ins, extra_ref, out_ref, rest_ref = refs[: len(widths)], refs[-3], refs[-2], refs[-1]
    total = sum(widths)
    fold = folds(total)
    full, rest = total // LANES, total % LANES
    lead = widths[0]
    assert full == lead // LANES
    for tile in range(full):
        out_ref[0, pl.ds(tile * rows, rows), :] = ins[0][:, tile * LANES : (tile + 1) * LANES]
    if rest:
        group = rows // fold
        splits = [lead - full * LANES] + list(widths[1:])
        for number, size in enumerate(splits):
            first = full * LANES if number == 0 else 0
            rest_ref[number, :, :size] = ins[number][:, first : first + size].astype(jnp.float32)

        def step(index, carry):
            pieces = []
            for part in range(fold):
                low = pl.multiple_of(part * group + index * SLAB, SLAB)
                for number, size in enumerate(splits):
                    pieces.append((rest_ref[number, pl.ds(low, SLAB), :], 0, size))
            for tile, value in enumerate(assemble(pieces)):
                low = pl.multiple_of(full * rows + tile * group + index * SLAB, SLAB)
                out_ref[0, pl.ds(low, SLAB), :] = value.astype(jnp.bfloat16)
            return carry

        lax.fori_loop(0, group // SLAB, step, 0)
    if extra:
        out_ref[0, pl.ds(tile_rows(rows, total), extra), :] = extra_ref[0]


def pack_columns(count, tensors, extra):
    rows = tensors[0].shape[0] // count
    widths = [tensor.shape[1] for tensor in tensors]
    body = tile_rows(rows, sum(widths))
    if not columns_fit(count, rows, sum(widths)):
        joined = jnp.concatenate(tensors, axis=1) if len(tensors) > 1 else tensors[0]
        flat = joined.reshape(count, -1, LANES)
        return jnp.concatenate([flat, jnp.broadcast_to(extra, (count,) + extra.shape[1:])], axis=1)
    extra_rows = extra.shape[1]
    shared = extra.shape[0] == 1
    return pl.pallas_call(
        functools.partial(pack_columns_kernel, widths, rows, extra_rows),
        grid=(count,),
        in_specs=[pl.BlockSpec((rows, width), lambda f: (f, 0)) for width in widths]
        + [
            pl.BlockSpec(
                (1, extra_rows, LANES), (lambda f: (0, 0, 0)) if shared else (lambda f: (f, 0, 0))
            )
        ],
        out_specs=pl.BlockSpec((1, body + extra_rows, LANES), lambda f: (f, 0, 0)),
        out_shape=jax.ShapeDtypeStruct((count, body + extra_rows, LANES), jnp.bfloat16),
        scratch_shapes=[pltpu.VMEM((len(widths), rows, LANES), jnp.float32)],
        cost_estimate=cost(count * body * LANES),
    )(*tensors, extra)


def pack_rows_kernel(rows, width, extra, in_ref, extra_ref, out_ref):
    full, half = width // LANES, rows // 2
    for side in range(2):
        if side == 0:
            for tile in range(full):
                out_ref[0, pl.ds(tile * rows, rows), :] = in_ref[
                    :, tile * LANES : (tile + 1) * LANES
                ]

        def step(index, carry):
            lasts = []
            for part in range(2):
                low = pl.multiple_of(part * half + index * SLAB, SLAB)
                values = [
                    in_ref[pl.ds(low, SLAB), tile * LANES : (tile + 1) * LANES].astype(jnp.float32)
                    for tile in range(side * full, side * full + full + 1)
                ]
                if side == 0:
                    lasts.append((values[full], 0, LANES // 2))
                else:
                    pieces = [(values[0], LANES // 2, LANES // 2)]
                    pieces += [(value, 0, LANES) for value in values[1:-1]]
                    pieces += [(values[-1], 0, LANES // 2)]
                    for tile, value in enumerate(assemble(pieces)):
                        to = pl.multiple_of(tile * rows + part * half + index * SLAB, SLAB)
                        out_ref[1, pl.ds(to, SLAB), :] = value.astype(jnp.bfloat16)
                    lasts.append((values[-1], LANES // 2, LANES // 2))
            to = pl.multiple_of(full * rows + index * SLAB, SLAB)
            out_ref[side, pl.ds(to, SLAB), :] = assemble(lasts)[0].astype(jnp.bfloat16)
            return carry

        lax.fori_loop(0, half // SLAB, step, 0)
        if extra:
            out_ref[side, pl.ds(tile_rows(rows, width), extra), :] = extra_ref[0]


def pack_rows(count, tensor, extra):
    rows = tensor.shape[0]
    width = tensor.shape[1] // count
    body = tile_rows(rows, width)
    extra_rows = extra.shape[1]
    if not rows_fit(count, rows, width):
        flat = tensor.reshape(rows, count, width).transpose(1, 0, 2).reshape(count, -1, LANES)
        return jnp.concatenate([flat, jnp.broadcast_to(extra, (count,) + extra.shape[1:])], axis=1)
    return pl.pallas_call(
        functools.partial(pack_rows_kernel, rows, width, extra_rows),
        grid=(count // 2,),
        in_specs=[
            pl.BlockSpec((rows, 2 * width), lambda f: (0, f)),
            pl.BlockSpec((1, extra_rows, LANES), lambda f: (0, 0, 0)),
        ],
        out_specs=pl.BlockSpec((2, body + extra_rows, LANES), lambda f: (f, 0, 0)),
        out_shape=jax.ShapeDtypeStruct((count, body + extra_rows, LANES), jnp.bfloat16),
        cost_estimate=cost(count * body * LANES),
    )(tensor, extra)


def unpack_columns_kernel(widths, numbers, rows, factor_ref, in_ref, *out_refs):
    total = sum(widths)
    fold = folds(total)
    group = rows // fold
    full, rest = total // LANES, total % LANES
    sources = in_ref.shape[0]
    for part in range(fold):

        def step(index, carry):
            pieces = [[] for _ in widths]
            low = pl.multiple_of(part * group + index * SLAB, SLAB)
            for source in range(sources):
                have = []
                for tile in range(full):
                    at = pl.multiple_of(tile * rows + part * group + index * SLAB, SLAB)
                    have.append((in_ref[source, pl.ds(at, SLAB), :].astype(jnp.float32), 0, LANES))
                first = part * rest
                while first < (part + 1) * rest:
                    tile = first // LANES
                    last = min((part + 1) * rest, (tile + 1) * LANES)
                    at = pl.multiple_of(full * rows + tile * group + index * SLAB, SLAB)
                    value = in_ref[source, pl.ds(at, SLAB), :].astype(jnp.float32)
                    have.append((value, first - tile * LANES, last - first))
                    first = last
                for number, width in enumerate(widths):
                    need = width
                    while need:
                        value, start, length = have.pop(0)
                        taken = min(need, length)
                        pieces[number].append((value, start, taken))
                        if taken < length:
                            have.insert(0, (value, start + taken, length - taken))
                        need -= taken
            for number, out_ref in enumerate(out_refs):
                factor = factor_ref[numbers[number]]
                for tile, value in enumerate(assemble(pieces[number])):
                    out_ref[pl.ds(low, SLAB), tile * LANES : (tile + 1) * LANES] = (
                        value * factor
                    ).astype(jnp.bfloat16)
            return carry

        lax.fori_loop(0, group // SLAB, step, 0)


def unpack_columns(count, arrived, rows, widths, factors, numbers):
    total = sum(widths)
    body = tile_rows(rows, total)
    if not columns_fit(count, rows, total):
        blocks = arrived[:, :body].reshape(count, rows, total)
        outs, low = [], 0
        for width, number in zip(widths, numbers):
            part = blocks[:, :, low : low + width].transpose(1, 0, 2).reshape(rows, count * width)
            outs.append(quantize(part, factors[number]))
            low += width
        return tuple(outs)
    sources = max(folds(width) for width in widths)
    return pl.pallas_call(
        functools.partial(unpack_columns_kernel, widths, numbers, rows),
        grid=(count // sources,),
        in_specs=[
            pl.BlockSpec(memory_space=pltpu.SMEM),
            pl.BlockSpec((sources, body, LANES), lambda g: (g, 0, 0)),
        ],
        out_specs=[pl.BlockSpec((rows, sources * width), lambda g: (0, g)) for width in widths],
        out_shape=[jax.ShapeDtypeStruct((rows, count * width), jnp.bfloat16) for width in widths],
        cost_estimate=cost(count * body * LANES),
    )(factors, arrived)


def unpack_rows_kernel(number, rows, width, factor_ref, in_ref, out_ref):
    full, half = width // LANES, rows // 2
    factor = factor_ref[number]
    for tile in range(full):
        value = in_ref[0, pl.ds(tile * rows, rows), :].astype(jnp.float32)
        out_ref[:, tile * LANES : (tile + 1) * LANES] = (value * factor).astype(jnp.bfloat16)
    last = in_ref[0, pl.ds(full * rows, half), :].astype(jnp.float32) * factor
    out_ref[pl.ds(0, half), full * LANES :] = last[:, : LANES // 2].astype(jnp.bfloat16)
    turned = pltpu.roll(last, LANES // 2, 1)
    out_ref[pl.ds(half, half), full * LANES :] = turned[:, : LANES // 2].astype(jnp.bfloat16)


def unpack_rows(count, arrived, rows, width, factors, number):
    body = tile_rows(rows, width)
    if not rows_fit(count, rows, width):
        return quantize(arrived[:, :body].reshape(count * rows, width), factors[number])
    return pl.pallas_call(
        functools.partial(unpack_rows_kernel, number, rows, width),
        grid=(count,),
        in_specs=[
            pl.BlockSpec(memory_space=pltpu.SMEM),
            pl.BlockSpec((1, body, LANES), lambda s: (s, 0, 0)),
        ],
        out_specs=pl.BlockSpec((rows, width), lambda s: (s, 0)),
        out_shape=jax.ShapeDtypeStruct((count * rows, width), jnp.bfloat16),
        cost_estimate=cost(count * body * LANES),
    )(factors, arrived)


def padded_rows(values, multiple):
    lead, size = values.shape
    unit = multiple * LANES
    room = -(-size // unit) * unit
    return jnp.pad(values, ((0, 0), (0, room - size))).reshape(lead, room // LANES, LANES)


def split_float(values):
    parts = []
    for _ in range(3):
        part = lax.reduce_precision(values, 8, 7)
        parts.append(part.astype(jnp.bfloat16))
        values = values - part
    return jnp.stack(parts)


def attend(query, key_new, value_new, key_cache, value_cache, lengths):
    count_seq = query.shape[0]
    kv_count = query.shape[1]
    head_dim = query.shape[3]
    cache_len = key_cache.shape[1]
    keys = key_cache.reshape(count_seq, cache_len, kv_count, head_dim)
    values = value_cache.reshape(count_seq, cache_len, kv_count, head_dim)
    scale = head_dim ** (-0.5)
    scores = jnp.einsum("bkgd,bjkd->bkgj", query, keys, preferred_element_type=jnp.float32) * scale
    own = (
        jnp.sum(query.astype(jnp.float32) * key_new.astype(jnp.float32)[:, :, None, :], axis=-1)
        * scale
    )
    valid = (lax.broadcasted_iota(jnp.int32, (count_seq, cache_len), 1) < lengths[:, None])[
        :, None, None, :
    ]
    top = jnp.maximum(jnp.max(jnp.where(valid, scores, -1e30), axis=-1), own)
    weights = jnp.where(valid, jnp.exp(scores - top[..., None]), 0.0)
    own_weight = jnp.exp(own - top)
    total = jnp.sum(weights, axis=-1) + own_weight
    probs = (weights / total[..., None]).astype(jnp.bfloat16)
    own_prob = (own_weight / total).astype(jnp.bfloat16)
    mixed = jnp.einsum("bkgj,bjkd->bkgd", probs, values, preferred_element_type=jnp.float32)
    mixed = (
        mixed
        + own_prob.astype(jnp.float32)[..., None] * value_new.astype(jnp.float32)[:, :, None, :]
    )
    return mixed.astype(jnp.bfloat16).reshape(count_seq, -1)


def per_device(
    hidden,
    query_weight,
    key_weight,
    value_weight,
    output_weight,
    gate_weight,
    up_weight,
    down_weight,
    history,
    slot,
    lengths,
    key_cache,
    value_cache,
):
    trainer = (
        query_weight,
        key_weight,
        value_weight,
        output_weight,
        gate_weight,
        up_weight,
        down_weight,
    )
    count = lax.axis_size("fsdp")
    model = query_weight.shape[0]
    rows = model // count
    seqs = hidden.shape[0]
    mine = lengths.shape[0]
    widths = [query_weight.shape[1], key_weight.shape[1], value_weight.shape[1]]
    group = query_weight.shape[1] // key_weight.shape[1]

    sent_hidden = hidden.reshape(1, -1, LANES)
    first = exchange(pack_rows(count, output_weight, sent_hidden))
    local = jnp.stack([largest(tensor) for tensor in trainer])
    sent_local = padded_rows(local[None, :].astype(jnp.bfloat16), SLAB)
    second = exchange(pack_columns(count, trainer[:3], sent_local), first)
    none = jnp.zeros((1, SLAB, LANES), jnp.bfloat16)
    third = exchange(pack_columns(count, (gate_weight,), none), second)

    body = tile_rows(rows, sum(widths))
    heard = second[:, body:].reshape(count, -1)[:, :7].astype(jnp.float32)
    peaks = lax.pmax(jnp.max(heard, axis=0), "tp")
    factors, new_history = scaling(peaks, history, slot)
    body = tile_rows(output_weight.shape[0], rows)
    whole_hidden = first[:, body:].reshape(count, seqs, rows).transpose(1, 0, 2)
    whole_hidden = whole_hidden.reshape(seqs, model)
    widened = whole_hidden.astype(jnp.float32)
    inv_rms = lax.rsqrt(jnp.mean(widened * widened, axis=1) + norm_eps)[:, None]
    fresh = jnp.concatenate(
        [
            jnp.dot(
                whole_hidden,
                quantize(trainer[number], factors[number]),
                preferred_element_type=jnp.float32,
            )
            * inv_rms
            / factors[number]
            for number in range(3)
        ],
        axis=1,
    )
    pieces = split_float(fresh).reshape(3, count, mine, -1).transpose(1, 0, 2, 3)
    sent_fresh = padded_rows(pieces.reshape(count, -1), SLAB)
    fourth = exchange(pack_columns(count, (up_weight,), sent_fresh), third)
    fifth = exchange(pack_columns(count, (down_weight.T,), none), fourth)

    query_rollout, key_rollout, value_rollout = unpack_columns(
        count, second, rows, widths, factors, (0, 1, 2)
    )
    output_rollout = unpack_rows(count, first, output_weight.shape[0], rows, factors, 3)
    (gate_rollout,) = unpack_columns(count, third, rows, [gate_weight.shape[1]], factors, (4,))
    (up_rollout,) = unpack_columns(count, fourth, rows, [up_weight.shape[1]], factors, (5,))
    (down_rollout,) = unpack_columns(count, fifth, rows, [down_weight.shape[0]], factors, (6,))
    down_rollout = down_rollout.T

    body = tile_rows(rows, up_weight.shape[1])
    heard = fourth[:, body:].reshape(count, -1)[:, : 3 * mine * sum(widths)]
    heard = heard.reshape(count, 3, mine, sum(widths)).astype(jnp.float32)
    heard = (heard[:, 0] + heard[:, 1]) + heard[:, 2]
    heard = heard.transpose(1, 0, 2)
    query = heard[:, :, : widths[0]].reshape(mine, -1, HEAD_DIM)
    key_new = heard[:, :, widths[0] : widths[0] + widths[1]].reshape(mine, -1, HEAD_DIM)
    value_new = heard[:, :, widths[0] + widths[1] :].reshape(mine, -1, HEAD_DIM)
    query = rotate(query, lengths).astype(jnp.bfloat16).reshape(mine, -1, group, HEAD_DIM)
    key_new = rotate(key_new, lengths).astype(jnp.bfloat16)
    attention_out = attend(
        query, key_new, value_new.astype(jnp.bfloat16), key_cache, value_cache, lengths
    )
    return (
        attention_out,
        query_rollout,
        key_rollout,
        value_rollout,
        output_rollout,
        gate_rollout,
        up_rollout,
        down_rollout,
        new_history,
    )


def solution(mesh):
    return jax.shard_map(
        per_device,
        mesh=mesh,
        in_specs=(
            P(None, "fsdp"),
            P(None, ("tp", "fsdp")),
            P(None, ("tp", "fsdp")),
            P(None, ("tp", "fsdp")),
            P(("tp", "fsdp"), None),
            P(None, ("tp", "fsdp")),
            P(None, ("tp", "fsdp")),
            P(("tp", "fsdp"), None),
            P(),
            P(),
            P("fsdp"),
            P("fsdp", None, "tp"),
            P("fsdp", None, "tp"),
        ),
        out_specs=(
            P("fsdp", "tp"),
            P("fsdp", "tp"),
            P("fsdp", "tp"),
            P("fsdp", "tp"),
            P("tp", "fsdp"),
            P("fsdp", "tp"),
            P("fsdp", "tp"),
            P("tp", "fsdp"),
            P(),
        ),
        check_vma=False,
    )
```

```python
import functools
import math

import jax
import jax.numpy as jnp
from jax import lax
from jax.experimental import pallas as pl
from jax.experimental.pallas import tpu as pltpu
from jax.sharding import PartitionSpec as P


HEAD_DIM = 128
LANES = 128
SLAB = 16


target_peak = 4.0
norm_eps = 1e-06
rope_theta = 1000000.0


def largest(tensor):
    return jnp.max(jnp.abs(tensor.astype(jnp.float32)))


def scaling(peaks, history, slot):
    marked = lax.broadcasted_iota(jnp.int32, history.shape, 1) == slot[0]
    kept = jnp.max(jnp.where(marked, jnp.zeros_like(history), history), axis=1)
    return (target_peak / jnp.maximum(peaks, kept), jnp.where(marked, peaks[:, None], history))


def quantize(tensor, factor):
    return (tensor.astype(jnp.float32) * factor).astype(jnp.bfloat16)


def rotate(vectors, positions):
    half_dim = vectors.shape[-1] // 2
    ladder = jnp.arange(half_dim, dtype=jnp.float32)
    spread = rope_theta ** (-2.0 * ladder / vectors.shape[-1])
    angle = positions.astype(jnp.float32)[:, None] * spread[None, :]
    cosine = jnp.cos(angle)[:, None, :]
    sine = jnp.sin(angle)[:, None, :]
    first = vectors[..., :half_dim]
    second = vectors[..., half_dim:]
    return jnp.concatenate(
        [first * cosine - second * sine, second * cosine + first * sine], axis=-1
    )


def after(tensor, *earlier):
    return lax.optimization_barrier((tensor,) + earlier)[0]


def exchange(blocks, *earlier):
    return lax.all_to_all(
        after(blocks, *earlier), "fsdp", split_axis=0, concat_axis=0, tiled=True
    )


def folds(width):
    rest = width % LANES
    return 1 if rest == 0 else LANES // math.gcd(rest, LANES)


def tile_rows(rows, width):
    return rows * width // LANES


def lane_index(rows):
    return lax.broadcasted_iota(jnp.int32, (rows, LANES), 1)


def assemble(pieces):
    total = sum(length for _, _, length in pieces)
    lanes = lane_index(pieces[0][0].shape[0])
    tiles = [None] * (total // LANES)
    offset = 0
    for value, start, length in pieces:
        shift = (offset - start) % LANES
        moved = pltpu.roll(value, shift, 1) if shift else value
        for tile in range(offset // LANES, (offset + length - 1) // LANES + 1):
            low = max(offset - tile * LANES, 0)
            old = tiles[tile]
            tiles[tile] = moved if low == 0 else jnp.where(lanes >= low, moved, old)
        offset += length
    return tiles


def slab_of(rows, limit):
    return max(slab for slab in range(SLAB, limit + 1, SLAB) if rows % slab == 0)


def cost(count):
    return pl.CostEstimate(flops=count, bytes_accessed=4 * count, transcendentals=0)


def columns_fit(count, rows, width):
    fold = folds(width)
    return rows % (SLAB * fold) == 0 and count % folds(width) == 0 and width >= 1


def rows_fit(count, rows, width):
    return count % 2 == 0 and width > LANES and width % LANES == LANES // 2 and rows % (2 * SLAB) == 0


def pack_columns_kernel(widths, rows, extra, *refs):
    ins, out_ref, rest_ref = refs[: len(widths)], refs[-2], refs[-1]
    total = sum(widths)
    fold = folds(total)
    full, rest = total // LANES, total % LANES
    lead = widths[0]
    assert full == lead // LANES
    for tile in range(full):
        out_ref[0, pl.ds(tile * rows, rows), :] = ins[0][:, tile * LANES : (tile + 1) * LANES]
    if rest:
        group = rows // fold
        slab = slab_of(group, 80)
        splits = [lead - full * LANES] + list(widths[1:])
        for number, size in enumerate(splits):
            first = full * LANES if number == 0 else 0
            rest_ref[number, :, :size] = ins[number][:, first : first + size].astype(jnp.float32)

        def step(index, carry):
            pieces = []
            for part in range(fold):
                low = pl.multiple_of(part * group + index * slab, SLAB)
                for number, size in enumerate(splits):
                    pieces.append((rest_ref[number, pl.ds(low, slab), :], 0, size))
            for tile, value in enumerate(assemble(pieces)):
                low = pl.multiple_of(full * rows + tile * group + index * slab, SLAB)
                out_ref[0, pl.ds(low, slab), :] = value.astype(jnp.bfloat16)
            return carry

        lax.fori_loop(0, group // slab, step, 0)
    if extra:
        out_ref[0, pl.ds(tile_rows(rows, total), extra), :] = refs[len(widths)][0]


def with_extra(count, flat, extra):
    if extra is None:
        return flat
    return jnp.concatenate([flat, jnp.broadcast_to(extra, (count,) + extra.shape[1:])], axis=1)


def pack_columns(count, tensors, extra=None):
    rows = tensors[0].shape[0] // count
    widths = [tensor.shape[1] for tensor in tensors]
    body = tile_rows(rows, sum(widths))
    if not columns_fit(count, rows, sum(widths)):
        joined = jnp.concatenate(tensors, axis=1) if len(tensors) > 1 else tensors[0]
        flat = joined.reshape(count, -1, LANES)
        return with_extra(count, flat, extra)
    extras = [] if extra is None else [extra]
    extra_rows = 0 if extra is None else extra.shape[1]
    return pl.pallas_call(
        functools.partial(pack_columns_kernel, widths, rows, extra_rows),
        grid=(count,),
        in_specs=[pl.BlockSpec((rows, width), lambda f: (f, 0)) for width in widths]
        + [pl.BlockSpec((1, extra_rows, LANES), lambda f: (0, 0, 0)) for _ in extras],
        out_specs=pl.BlockSpec((1, body + extra_rows, LANES), lambda f: (f, 0, 0)),
        out_shape=jax.ShapeDtypeStruct((count, body + extra_rows, LANES), jnp.bfloat16),
        scratch_shapes=[pltpu.VMEM((len(widths), rows, LANES), jnp.float32)],
        cost_estimate=cost(count * body * LANES),
    )(*tensors, *extras)


def pack_rows_kernel(rows, width, extra, in_ref, extra_ref, out_ref):
    full, half = width // LANES, rows // 2
    slab = slab_of(half, 80)
    for side in range(2):
        if side == 0:
            for tile in range(full):
                out_ref[0, pl.ds(tile * rows, rows), :] = in_ref[
                    :, tile * LANES : (tile + 1) * LANES
                ]

        def step(index, carry):
            lasts = []
            for part in range(2):
                low = pl.multiple_of(part * half + index * slab, SLAB)
                values = [
                    in_ref[pl.ds(low, slab), tile * LANES : (tile + 1) * LANES].astype(jnp.float32)
                    for tile in range(side * full, side * full + full + 1)
                ]
                if side == 0:
                    lasts.append((values[full], 0, LANES // 2))
                else:
                    pieces = [(values[0], LANES // 2, LANES // 2)]
                    pieces += [(value, 0, LANES) for value in values[1:-1]]
                    pieces += [(values[-1], 0, LANES // 2)]
                    for tile, value in enumerate(assemble(pieces)):
                        to = pl.multiple_of(tile * rows + part * half + index * slab, SLAB)
                        out_ref[1, pl.ds(to, slab), :] = value.astype(jnp.bfloat16)
                    lasts.append((values[-1], LANES // 2, LANES // 2))
            to = pl.multiple_of(full * rows + index * slab, SLAB)
            out_ref[side, pl.ds(to, slab), :] = assemble(lasts)[0].astype(jnp.bfloat16)
            return carry

        lax.fori_loop(0, half // slab, step, 0)
        if extra:
            out_ref[side, pl.ds(tile_rows(rows, width), extra), :] = extra_ref[0]


def pack_rows(count, tensor, extra):
    rows = tensor.shape[0]
    width = tensor.shape[1] // count
    body = tile_rows(rows, width)
    extra_rows = extra.shape[1]
    if not rows_fit(count, rows, width):
        flat = tensor.reshape(rows, count, width).transpose(1, 0, 2).reshape(count, -1, LANES)
        return with_extra(count, flat, extra)
    return pl.pallas_call(
        functools.partial(pack_rows_kernel, rows, width, extra_rows),
        grid=(count // 2,),
        in_specs=[
            pl.BlockSpec((rows, 2 * width), lambda f: (0, f)),
            pl.BlockSpec((1, extra_rows, LANES), lambda f: (0, 0, 0)),
        ],
        out_specs=pl.BlockSpec((2, body + extra_rows, LANES), lambda f: (f, 0, 0)),
        out_shape=jax.ShapeDtypeStruct((count, body + extra_rows, LANES), jnp.bfloat16),
        cost_estimate=cost(count * body * LANES),
    )(tensor, extra)


def unpack_columns_kernel(widths, numbers, rows, factor_ref, in_ref, *out_refs):
    total = sum(widths)
    fold = folds(total)
    group = rows // fold
    full, rest = total // LANES, total % LANES
    sources = in_ref.shape[0]
    for part in range(fold):

        def step(index, carry):
            pieces = [[] for _ in widths]
            low = part * group + index * SLAB
            for source in range(sources):
                have = []
                for tile in range(full):
                    at = tile * rows + part * group + index * SLAB
                    have.append((in_ref[source, pl.ds(at, SLAB), :].astype(jnp.float32), 0, LANES))
                first = part * rest
                while first < (part + 1) * rest:
                    tile = first // LANES
                    last = min((part + 1) * rest, (tile + 1) * LANES)
                    at = full * rows + tile * group + index * SLAB
                    value = in_ref[source, pl.ds(at, SLAB), :].astype(jnp.float32)
                    have.append((value, first - tile * LANES, last - first))
                    first = last
                for number, width in enumerate(widths):
                    need = width
                    while need:
                        value, start, length = have.pop(0)
                        taken = min(need, length)
                        pieces[number].append((value, start, taken))
                        if taken < length:
                            have.insert(0, (value, start + taken, length - taken))
                        need -= taken
            for number, out_ref in enumerate(out_refs):
                factor = factor_ref[numbers[number]]
                for tile, value in enumerate(assemble(pieces[number])):
                    out_ref[pl.ds(low, SLAB), tile * LANES : (tile + 1) * LANES] = (
                        value * factor
                    ).astype(jnp.bfloat16)
            return carry

        for index in range(group // SLAB):
            step(index, 0)


def unpack_columns(count, arrived, rows, widths, factors, numbers):
    total = sum(widths)
    body = tile_rows(rows, total)
    if not columns_fit(count, rows, total):
        blocks = arrived[:, :body].reshape(count, rows, total)
        outs, low = [], 0
        for width, number in zip(widths, numbers):
            part = blocks[:, :, low : low + width].transpose(1, 0, 2).reshape(rows, count * width)
            outs.append(quantize(part, factors[number]))
            low += width
        return tuple(outs)
    sources = max(folds(width) for width in widths)
    return pl.pallas_call(
        functools.partial(unpack_columns_kernel, widths, numbers, rows),
        grid=(count // sources,),
        in_specs=[
            pl.BlockSpec(memory_space=pltpu.SMEM),
            pl.BlockSpec((sources, body, LANES), lambda g: (g, 0, 0)),
        ],
        out_specs=[pl.BlockSpec((rows, sources * width), lambda g: (0, g)) for width in widths],
        out_shape=[jax.ShapeDtypeStruct((rows, count * width), jnp.bfloat16) for width in widths],
        cost_estimate=cost(count * body * LANES),
    )(factors, arrived)


def unpack_rows_kernel(number, rows, width, factor_ref, in_ref, out_ref):
    full, half = width // LANES, rows // 2
    factor = factor_ref[number]
    for tile in range(full):
        value = in_ref[0, pl.ds(tile * rows, rows), :].astype(jnp.float32)
        out_ref[:, tile * LANES : (tile + 1) * LANES] = (value * factor).astype(jnp.bfloat16)
    last = in_ref[0, pl.ds(full * rows, half), :].astype(jnp.float32) * factor
    out_ref[pl.ds(0, half), full * LANES :] = last[:, : LANES // 2].astype(jnp.bfloat16)
    turned = pltpu.roll(last, LANES // 2, 1)
    out_ref[pl.ds(half, half), full * LANES :] = turned[:, : LANES // 2].astype(jnp.bfloat16)


def unpack_rows(count, arrived, rows, width, factors, number):
    body = tile_rows(rows, width)
    if not rows_fit(count, rows, width):
        return quantize(arrived[:, :body].reshape(count * rows, width), factors[number])
    return pl.pallas_call(
        functools.partial(unpack_rows_kernel, number, rows, width),
        grid=(count,),
        in_specs=[
            pl.BlockSpec(memory_space=pltpu.SMEM),
            pl.BlockSpec((1, body, LANES), lambda s: (s, 0, 0)),
        ],
        out_specs=pl.BlockSpec((rows, width), lambda s: (s, 0)),
        out_shape=jax.ShapeDtypeStruct((count * rows, width), jnp.bfloat16),
        cost_estimate=cost(count * body * LANES),
    )(factors, arrived)


def padded_rows(values, multiple):
    lead, size = values.shape
    unit = multiple * LANES
    room = -(-size // unit) * unit
    return jnp.pad(values, ((0, 0), (0, room - size))).reshape(lead, room // LANES, LANES)


def shifted(block_for, steps):
    count = lax.axis_size("fsdp")
    here = lax.axis_index("fsdp")
    return {
        step: lax.ppermute(
            block_for((here + step) % count),
            "fsdp",
            [(place, (place + step) % count) for place in range(count)],
        )
        for step in steps
    }


def by_source(own, received):
    count = lax.axis_size("fsdp")
    blocks = jnp.stack([received[step] for step in range(count - 1, 0, -1)] + [own])
    twice = jnp.concatenate([blocks, blocks])
    return lax.dynamic_slice_in_dim(twice, count - 1 - lax.axis_index("fsdp"), count)


def maxima_kernel(*refs):
    ins, out_ref, seen_ref = refs[:-2], refs[-2], refs[-1]
    step = pl.program_id(0)
    for number, in_ref in enumerate(ins):
        sizes = jnp.abs(in_ref[...])
        rows, width = sizes.shape
        most = jnp.max(sizes.reshape(rows // SLAB, SLAB, width), axis=0).astype(jnp.float32)
        tiles = [most[:, low : low + LANES] for low in range(0, width, LANES)]
        best = functools.reduce(jnp.maximum, tiles)
        seen_ref[number] = jnp.where(step == 0, best, jnp.maximum(seen_ref[number], best))

    @pl.when(step == pl.num_programs(0) - 1)
    def _():
        lanes = lane_index(SLAB)
        total = jnp.zeros((SLAB, LANES), jnp.float32)
        for number in range(len(ins)):
            total = jnp.where(lanes == number, jnp.max(seen_ref[number]), total)
        out_ref[0] = total.astype(jnp.bfloat16)


def maxima(tensors):
    blocks = 8
    width = tensors[0].shape[1] // blocks
    if width % LANES or any(tensor.shape[0] % SLAB for tensor in tensors):
        local = jnp.stack([largest(tensor) for tensor in tensors])
        return padded_rows(local[None, :].astype(jnp.bfloat16), SLAB)
    return pl.pallas_call(
        maxima_kernel,
        grid=(blocks,),
        in_specs=[pl.BlockSpec((tensor.shape[0], width), lambda f: (0, f)) for tensor in tensors],
        out_specs=pl.BlockSpec((1, SLAB, LANES), lambda f: (0, 0, 0)),
        out_shape=jax.ShapeDtypeStruct((1, SLAB, LANES), jnp.bfloat16),
        scratch_shapes=[pltpu.VMEM((len(tensors), SLAB, LANES), jnp.float32)],
        cost_estimate=cost(sum(tensor.size for tensor in tensors) // 2),
    )(*tensors)


def attend(query, key_new, value_new, key_cache, value_cache, lengths):
    count_seq = query.shape[0]
    kv_count = query.shape[1]
    head_dim = query.shape[3]
    cache_len = key_cache.shape[1]
    keys = key_cache.reshape(count_seq, cache_len, kv_count, head_dim)
    values = value_cache.reshape(count_seq, cache_len, kv_count, head_dim)
    scale = head_dim ** (-0.5)
    scores = jnp.einsum("bkgd,bjkd->bkgj", query, keys, preferred_element_type=jnp.float32) * scale
    own = (
        jnp.sum(query.astype(jnp.float32) * key_new.astype(jnp.float32)[:, :, None, :], axis=-1)
        * scale
    )
    valid = (lax.broadcasted_iota(jnp.int32, (count_seq, cache_len), 1) < lengths[:, None])[
        :, None, None, :
    ]
    top = jnp.maximum(jnp.max(jnp.where(valid, scores, -1e30), axis=-1), own)
    weights = jnp.where(valid, jnp.exp(scores - top[..., None]), 0.0)
    own_weight = jnp.exp(own - top)
    total = jnp.sum(weights, axis=-1) + own_weight
    probs = (weights / total[..., None]).astype(jnp.bfloat16)
    own_prob = (own_weight / total).astype(jnp.bfloat16)
    mixed = jnp.einsum("bkgj,bjkd->bkgd", probs, values, preferred_element_type=jnp.float32)
    mixed = (
        mixed
        + own_prob.astype(jnp.float32)[..., None] * value_new.astype(jnp.float32)[:, :, None, :]
    )
    return mixed.astype(jnp.bfloat16).reshape(count_seq, -1)


def per_device(
    hidden,
    query_weight,
    key_weight,
    value_weight,
    output_weight,
    gate_weight,
    up_weight,
    down_weight,
    history,
    slot,
    lengths,
    key_cache,
    value_cache,
):
    trainer = (
        query_weight,
        key_weight,
        value_weight,
        output_weight,
        gate_weight,
        up_weight,
        down_weight,
    )
    count = lax.axis_size("fsdp")
    model = query_weight.shape[0]
    rows = model // count
    seqs = hidden.shape[0]
    mine = lengths.shape[0]
    widths = [query_weight.shape[1], key_weight.shape[1], value_weight.shape[1]]
    group = query_weight.shape[1] // key_weight.shape[1]

    sent_hidden = hidden.reshape(1, -1, LANES)
    first = exchange(pack_rows(count, output_weight, sent_hidden))
    packed = pack_columns(count, trainer[:3])

    def block_of(blocks):
        return lambda device: lax.dynamic_index_in_dim(blocks, device, 0, keepdims=False)

    received = {}
    steps = range(1, count)
    bridges = [count // 2, count // 2 - 1, count // 2 + 1, count // 2 - 2]
    received |= shifted(block_of(packed), [step for step in steps if step not in bridges])
    flat = [tensor.T for tensor in trainer]
    flat[3], flat[6] = output_weight, down_weight
    sent = pack_rows(count, down_weight, maxima(flat))
    second = exchange(sent, first)
    ready = after(packed, first)
    received |= shifted(block_of(ready), bridges[:2])
    sent = pack_columns(count, (after(up_weight, first),))
    third = exchange(sent, second)
    ready = after(packed, second)
    received |= shifted(block_of(ready), bridges[2:])

    body = tile_rows(down_weight.shape[0], rows)
    heard = second[:, body:].reshape(count, -1)[:, :7].astype(jnp.float32)
    peaks = lax.pmax(jnp.max(heard, axis=0), "tp")
    factors, new_history = scaling(peaks, history, slot)
    body = tile_rows(output_weight.shape[0], rows)
    whole_hidden = first[:, body:].reshape(count, seqs, rows).transpose(1, 0, 2)
    whole_hidden = whole_hidden.reshape(seqs, model)
    widened = whole_hidden.astype(jnp.float32)
    inv_rms = lax.rsqrt(jnp.mean(widened * widened, axis=1) + norm_eps)[:, None]
    fresh = jnp.concatenate(
        [
            jnp.dot(
                whole_hidden,
                quantize(trainer[number], factors[number]),
                preferred_element_type=jnp.float32,
            )
            * inv_rms
            / factors[number]
            for number in range(3)
        ],
        axis=1,
    )
    fresh = fresh.reshape(count, mine, -1)
    heard = by_source(
        block_of(fresh)(lax.axis_index("fsdp")), shifted(block_of(fresh), steps)
    )
    sent = pack_columns(count, (after(gate_weight, second),))
    fourth = exchange(sent, third)

    heard = heard.transpose(1, 0, 2)
    query = heard[:, :, : widths[0]].reshape(mine, -1, HEAD_DIM)
    key_new = heard[:, :, widths[0] : widths[0] + widths[1]].reshape(mine, -1, HEAD_DIM)
    value_new = heard[:, :, widths[0] + widths[1] :].reshape(mine, -1, HEAD_DIM)
    query = rotate(query, lengths).astype(jnp.bfloat16).reshape(mine, -1, group, HEAD_DIM)
    key_new = rotate(key_new, lengths).astype(jnp.bfloat16)
    attention_out = attend(
        query, key_new, value_new.astype(jnp.bfloat16), key_cache, value_cache, lengths
    )
    output_rollout = unpack_rows(count, first, output_weight.shape[0], rows, factors, 3)
    down_rollout = unpack_rows(count, second, down_weight.shape[0], rows, factors, 6)
    (gate_rollout,) = unpack_columns(count, fourth, rows, [gate_weight.shape[1]], factors, (4,))
    (up_rollout,) = unpack_columns(count, third, rows, [up_weight.shape[1]], factors, (5,))
    received = lax.optimization_barrier((received, attention_out))[0]
    arrived = by_source(block_of(packed)(lax.axis_index("fsdp")), received)
    query_rollout, key_rollout, value_rollout = unpack_columns(
        count, arrived, rows, widths, factors, (0, 1, 2)
    )
    return (
        attention_out,
        query_rollout,
        key_rollout,
        value_rollout,
        output_rollout,
        gate_rollout,
        up_rollout,
        down_rollout,
        new_history,
    )


def solution(mesh):
    return jax.shard_map(
        per_device,
        mesh=mesh,
        in_specs=(
            P(None, "fsdp"),
            P(None, ("tp", "fsdp")),
            P(None, ("tp", "fsdp")),
            P(None, ("tp", "fsdp")),
            P(("tp", "fsdp"), None),
            P(None, ("tp", "fsdp")),
            P(None, ("tp", "fsdp")),
            P(("tp", "fsdp"), None),
            P(),
            P(),
            P("fsdp"),
            P("fsdp", None, "tp"),
            P("fsdp", None, "tp"),
        ),
        out_specs=(
            P("fsdp", "tp"),
            P("fsdp", "tp"),
            P("fsdp", "tp"),
            P("fsdp", "tp"),
            P("tp", "fsdp"),
            P("fsdp", "tp"),
            P("fsdp", "tp"),
            P("tp", "fsdp"),
            P(),
        ),
        check_vma=False,
    )
```

```python
import functools
import math

import jax
import jax.numpy as jnp
from jax import lax
from jax.experimental import pallas as pl
from jax.experimental.pallas import tpu as pltpu
from jax.sharding import PartitionSpec as P


HEAD_DIM = 128
LANES = 128
SLAB = 16


target_peak = 4.0
norm_eps = 1e-06
rope_theta = 1000000.0


def largest(tensor):
    return jnp.max(jnp.abs(tensor.astype(jnp.float32)))


def scaling(peaks, history, slot):
    marked = lax.broadcasted_iota(jnp.int32, history.shape, 1) == slot[0]
    kept = jnp.max(jnp.where(marked, jnp.zeros_like(history), history), axis=1)
    return (target_peak / jnp.maximum(peaks, kept), jnp.where(marked, peaks[:, None], history))


def quantize(tensor, factor):
    return (tensor.astype(jnp.float32) * factor).astype(jnp.bfloat16)


def rotate(vectors, positions):
    half_dim = vectors.shape[-1] // 2
    ladder = jnp.arange(half_dim, dtype=jnp.float32)
    spread = rope_theta ** (-2.0 * ladder / vectors.shape[-1])
    angle = positions.astype(jnp.float32)[:, None] * spread[None, :]
    cosine = jnp.cos(angle)[:, None, :]
    sine = jnp.sin(angle)[:, None, :]
    first = vectors[..., :half_dim]
    second = vectors[..., half_dim:]
    return jnp.concatenate(
        [first * cosine - second * sine, second * cosine + first * sine], axis=-1
    )


def after(tensor, *earlier):
    return lax.optimization_barrier((tensor,) + earlier)[0]


def exchange(blocks, *earlier):
    return lax.all_to_all(
        after(blocks, *earlier), "fsdp", split_axis=0, concat_axis=0, tiled=True
    )


def folds(width):
    rest = width % LANES
    return 1 if rest == 0 else LANES // math.gcd(rest, LANES)


def tile_rows(rows, width):
    return rows * width // LANES


def lane_index(rows):
    return lax.broadcasted_iota(jnp.int32, (rows, LANES), 1)


def assemble(pieces):
    total = sum(length for _, _, length in pieces)
    lanes = lane_index(pieces[0][0].shape[0])
    tiles = [None] * (total // LANES)
    offset = 0
    for value, start, length in pieces:
        shift = (offset - start) % LANES
        moved = pltpu.roll(value, shift, 1) if shift else value
        for tile in range(offset // LANES, (offset + length - 1) // LANES + 1):
            low = max(offset - tile * LANES, 0)
            old = tiles[tile]
            tiles[tile] = moved if low == 0 else jnp.where(lanes >= low, moved, old)
        offset += length
    return tiles


def slab_of(rows, limit):
    return max(slab for slab in range(SLAB, limit + 1, SLAB) if rows % slab == 0)


def cost(count):
    return pl.CostEstimate(flops=count, bytes_accessed=4 * count, transcendentals=0)


def columns_fit(count, rows, width):
    fold = folds(width)
    return rows % (SLAB * fold) == 0 and count % folds(width) == 0 and width >= 1


def rows_fit(count, rows, width):
    return count % 2 == 0 and width > LANES and width % LANES == LANES // 2 and rows % (2 * SLAB) == 0


def pack_columns_kernel(widths, rows, extra, *refs):
    ins, out_ref, rest_ref = refs[: len(widths)], refs[-2], refs[-1]
    total = sum(widths)
    fold = folds(total)
    full, rest = total // LANES, total % LANES
    lead = widths[0]
    assert full == lead // LANES
    for tile in range(full):
        out_ref[0, pl.ds(tile * rows, rows), :] = ins[0][:, tile * LANES : (tile + 1) * LANES]
    if rest:
        group = rows // fold
        slab = slab_of(group, 80)
        splits = [lead - full * LANES] + list(widths[1:])
        for number, size in enumerate(splits):
            first = full * LANES if number == 0 else 0
            rest_ref[number, :, :size] = ins[number][:, first : first + size].astype(jnp.float32)

        def step(index, carry):
            pieces = []
            for part in range(fold):
                low = pl.multiple_of(part * group + index * slab, SLAB)
                for number, size in enumerate(splits):
                    pieces.append((rest_ref[number, pl.ds(low, slab), :], 0, size))
            for tile, value in enumerate(assemble(pieces)):
                low = pl.multiple_of(full * rows + tile * group + index * slab, SLAB)
                out_ref[0, pl.ds(low, slab), :] = value.astype(jnp.bfloat16)
            return carry

        lax.fori_loop(0, group // slab, step, 0)
    if extra:
        out_ref[0, pl.ds(tile_rows(rows, total), extra), :] = refs[len(widths)][0]


def with_extra(count, flat, extra):
    if extra is None:
        return flat
    return jnp.concatenate([flat, jnp.broadcast_to(extra, (count,) + extra.shape[1:])], axis=1)


def pack_columns(count, tensors, extra=None):
    rows = tensors[0].shape[0] // count
    widths = [tensor.shape[1] for tensor in tensors]
    body = tile_rows(rows, sum(widths))
    if not columns_fit(count, rows, sum(widths)):
        joined = jnp.concatenate(tensors, axis=1) if len(tensors) > 1 else tensors[0]
        flat = joined.reshape(count, -1, LANES)
        return with_extra(count, flat, extra)
    extras = [] if extra is None else [extra]
    extra_rows = 0 if extra is None else extra.shape[1]
    return pl.pallas_call(
        functools.partial(pack_columns_kernel, widths, rows, extra_rows),
        grid=(count,),
        in_specs=[pl.BlockSpec((rows, width), lambda f: (f, 0)) for width in widths]
        + [pl.BlockSpec((1, extra_rows, LANES), lambda f: (0, 0, 0)) for _ in extras],
        out_specs=pl.BlockSpec((1, body + extra_rows, LANES), lambda f: (f, 0, 0)),
        out_shape=jax.ShapeDtypeStruct((count, body + extra_rows, LANES), jnp.bfloat16),
        scratch_shapes=[pltpu.VMEM((len(widths), rows, LANES), jnp.float32)],
        cost_estimate=cost(count * body * LANES),
    )(*tensors, *extras)


def pack_rows_pair(rows, width, extra, in_ref, out_ref, *refs):
    full, half = width // LANES, rows // 2
    slab = slab_of(half, 80)
    for side in range(2):
        if side == 0:
            for tile in range(full):
                out_ref[0, pl.ds(tile * rows, rows), :] = in_ref[
                    :, tile * LANES : (tile + 1) * LANES
                ]

        def step(index, carry):
            lasts = []
            for part in range(2):
                low = part * half + index * slab
                values = [
                    in_ref[pl.ds(low, slab), tile * LANES : (tile + 1) * LANES].astype(jnp.float32)
                    for tile in range(side * full, side * full + full + 1)
                ]
                if side == 0:
                    lasts.append((values[full], 0, LANES // 2))
                else:
                    pieces = [(values[0], LANES // 2, LANES // 2)]
                    pieces += [(value, 0, LANES) for value in values[1:-1]]
                    pieces += [(values[-1], 0, LANES // 2)]
                    for tile, value in enumerate(assemble(pieces)):
                        to = tile * rows + part * half + index * slab
                        out_ref[1, pl.ds(to, slab), :] = value.astype(jnp.bfloat16)
                    lasts.append((values[-1], LANES // 2, LANES // 2))
            to = full * rows + index * slab
            out_ref[side, pl.ds(to, slab), :] = assemble(lasts)[0].astype(jnp.bfloat16)
            return carry

        for index in range(half // slab):
            step(index, 0)
        if extra:
            out_ref[side, pl.ds(tile_rows(rows, width), extra), :] = refs[0][0]


def pack_rows_kernel(rows, width, pairs, extra, in_ref, *refs):
    for pair in range(pairs):
        part = in_ref.at[:, pair * 2 * width : (pair + 1) * 2 * width]
        pack_rows_pair(rows, width, extra, part, refs[-1].at[pl.ds(2 * pair, 2)], *refs[:-1])


def pack_rows(count, tensor, extra=None):
    rows = tensor.shape[0]
    width = tensor.shape[1] // count
    body = tile_rows(rows, width)
    extras = [] if extra is None else [extra]
    extra_rows = 0 if extra is None else extra.shape[1]
    if not rows_fit(count, rows, width):
        flat = tensor.reshape(rows, count, width).transpose(1, 0, 2).reshape(count, -1, LANES)
        return with_extra(count, flat, extra)
    pairs = next(
        pairs
        for pairs in range(count // 2, 0, -1)
        if count // 2 % pairs == 0 and (pairs == 1 or pairs * 4 * rows * width <= 2**19)
    )
    return pl.pallas_call(
        functools.partial(pack_rows_kernel, rows, width, pairs, extra_rows),
        grid=(count // 2 // pairs,),
        in_specs=[
            pl.BlockSpec((rows, 2 * pairs * width), lambda f: (0, f)),
            *[pl.BlockSpec((1, extra_rows, LANES), lambda f: (0, 0, 0)) for _ in extras],
        ],
        out_specs=pl.BlockSpec((2 * pairs, body + extra_rows, LANES), lambda f: (f, 0, 0)),
        out_shape=jax.ShapeDtypeStruct((count, body + extra_rows, LANES), jnp.bfloat16),
        cost_estimate=cost(count * body * LANES),
    )(tensor, *extras)


def unpack_columns_kernel(widths, numbers, rows, factor_ref, in_ref, *out_refs):
    total = sum(widths)
    fold = folds(total)
    group = rows // fold
    full, rest = total // LANES, total % LANES
    sources = in_ref.shape[0]
    for part in range(fold):

        def step(index, carry):
            pieces = [[] for _ in widths]
            low = part * group + index * SLAB
            for source in range(sources):
                have = []
                for tile in range(full):
                    at = tile * rows + part * group + index * SLAB
                    have.append((in_ref[source, pl.ds(at, SLAB), :].astype(jnp.float32), 0, LANES))
                first = part * rest
                while first < (part + 1) * rest:
                    tile = first // LANES
                    last = min((part + 1) * rest, (tile + 1) * LANES)
                    at = full * rows + tile * group + index * SLAB
                    value = in_ref[source, pl.ds(at, SLAB), :].astype(jnp.float32)
                    have.append((value, first - tile * LANES, last - first))
                    first = last
                for number, width in enumerate(widths):
                    need = width
                    while need:
                        value, start, length = have.pop(0)
                        taken = min(need, length)
                        pieces[number].append((value, start, taken))
                        if taken < length:
                            have.insert(0, (value, start + taken, length - taken))
                        need -= taken
            for number, out_ref in enumerate(out_refs):
                factor = factor_ref[numbers[number]]
                for tile, value in enumerate(assemble(pieces[number])):
                    out_ref[pl.ds(low, SLAB), tile * LANES : (tile + 1) * LANES] = (
                        value * factor
                    ).astype(jnp.bfloat16)
            return carry

        for index in range(group // SLAB):
            step(index, 0)


def unpack_columns(count, arrived, rows, widths, factors, numbers):
    total = sum(widths)
    body = tile_rows(rows, total)
    if not columns_fit(count, rows, total):
        blocks = arrived[:, :body].reshape(count, rows, total)
        outs, low = [], 0
        for width, number in zip(widths, numbers):
            part = blocks[:, :, low : low + width].transpose(1, 0, 2).reshape(rows, count * width)
            outs.append(quantize(part, factors[number]))
            low += width
        return tuple(outs)
    sources = max(folds(width) for width in widths)
    return pl.pallas_call(
        functools.partial(unpack_columns_kernel, widths, numbers, rows),
        grid=(count // sources,),
        in_specs=[
            pl.BlockSpec(memory_space=pltpu.SMEM),
            pl.BlockSpec((sources, body, LANES), lambda g: (g, 0, 0)),
        ],
        out_specs=[pl.BlockSpec((rows, sources * width), lambda g: (0, g)) for width in widths],
        out_shape=[jax.ShapeDtypeStruct((rows, count * width), jnp.bfloat16) for width in widths],
        cost_estimate=cost(count * body * LANES),
    )(factors, arrived)


def unpack_rows_kernel(number, rows, width, factor_ref, in_ref, out_ref):
    full, half = width // LANES, rows // 2
    factor = factor_ref[number]
    for tile in range(full):
        value = in_ref[0, pl.ds(tile * rows, rows), :].astype(jnp.float32)
        out_ref[:, tile * LANES : (tile + 1) * LANES] = (value * factor).astype(jnp.bfloat16)
    last = in_ref[0, pl.ds(full * rows, half), :].astype(jnp.float32) * factor
    out_ref[pl.ds(0, half), full * LANES :] = last[:, : LANES // 2].astype(jnp.bfloat16)
    turned = pltpu.roll(last, LANES // 2, 1)
    out_ref[pl.ds(half, half), full * LANES :] = turned[:, : LANES // 2].astype(jnp.bfloat16)


def unpack_rows(count, arrived, rows, width, factors, number):
    body = tile_rows(rows, width)
    if not rows_fit(count, rows, width):
        return quantize(arrived[:, :body].reshape(count * rows, width), factors[number])
    return pl.pallas_call(
        functools.partial(unpack_rows_kernel, number, rows, width),
        grid=(count,),
        in_specs=[
            pl.BlockSpec(memory_space=pltpu.SMEM),
            pl.BlockSpec((1, body, LANES), lambda s: (s, 0, 0)),
        ],
        out_specs=pl.BlockSpec((rows, width), lambda s: (s, 0)),
        out_shape=jax.ShapeDtypeStruct((count * rows, width), jnp.bfloat16),
        cost_estimate=cost(count * body * LANES),
    )(factors, arrived)


def padded_rows(values, multiple):
    lead, size = values.shape
    unit = multiple * LANES
    room = -(-size // unit) * unit
    return jnp.pad(values, ((0, 0), (0, room - size))).reshape(lead, room // LANES, LANES)


def shifted(block_for, steps):
    count = lax.axis_size("fsdp")
    here = lax.axis_index("fsdp")
    return {
        step: lax.ppermute(
            block_for((here + step) % count),
            "fsdp",
            [(place, (place + step) % count) for place in range(count)],
        )
        for step in steps
    }


def by_source(own, received, stride=1):
    places = lax.axis_size("fsdp") // stride
    blocks = jnp.stack([received[stride * step] for step in range(places - 1, 0, -1)] + [own])
    twice = jnp.concatenate([blocks, blocks])
    return lax.dynamic_slice_in_dim(twice, places - 1 - lax.axis_index("fsdp") // stride, places)


def from_all(own, received):
    count = lax.axis_size("fsdp")
    same = by_source(own, received, 2)
    other = lax.ppermute(same, "fsdp", [(place, place ^ 1) for place in range(count)])
    even = lax.axis_index("fsdp") % 2 == 0
    pairs = jnp.stack([jnp.where(even, same, other), jnp.where(even, other, same)], axis=1)
    return pairs.reshape((count,) + own.shape)


def maxima_kernel(*refs):
    ins, out_ref, seen_ref = refs[:-2], refs[-2], refs[-1]
    step = pl.program_id(0)
    for number, in_ref in enumerate(ins):
        sizes = jnp.abs(in_ref[...])
        rows, width = sizes.shape
        most = jnp.max(sizes.reshape(rows // SLAB, SLAB, width), axis=0).astype(jnp.float32)
        tiles = [most[:, low : low + LANES] for low in range(0, width, LANES)]
        best = functools.reduce(jnp.maximum, tiles)
        seen_ref[number] = jnp.where(step == 0, best, jnp.maximum(seen_ref[number], best))

    @pl.when(step == pl.num_programs(0) - 1)
    def _():
        lanes = lane_index(SLAB)
        total = jnp.zeros((SLAB, LANES), jnp.float32)
        for number in range(len(ins)):
            total = jnp.where(lanes == number, jnp.max(seen_ref[number]), total)
        out_ref[0] = total.astype(jnp.bfloat16)


def maxima(tensors):
    blocks = 8
    width = tensors[0].shape[1] // blocks
    if width % LANES or any(tensor.shape[0] % SLAB for tensor in tensors):
        local = jnp.stack([largest(tensor) for tensor in tensors])
        return padded_rows(local[None, :].astype(jnp.bfloat16), SLAB)
    return pl.pallas_call(
        maxima_kernel,
        grid=(blocks,),
        in_specs=[pl.BlockSpec((tensor.shape[0], width), lambda f: (0, f)) for tensor in tensors],
        out_specs=pl.BlockSpec((1, SLAB, LANES), lambda f: (0, 0, 0)),
        out_shape=jax.ShapeDtypeStruct((1, SLAB, LANES), jnp.bfloat16),
        scratch_shapes=[pltpu.VMEM((len(tensors), SLAB, LANES), jnp.float32)],
        cost_estimate=cost(sum(tensor.size for tensor in tensors) // 2),
    )(*tensors)


def attend(query, key_new, value_new, key_cache, value_cache, lengths):
    count_seq = query.shape[0]
    kv_count = query.shape[1]
    head_dim = query.shape[3]
    cache_len = key_cache.shape[1]
    keys = key_cache.reshape(count_seq, cache_len, kv_count, head_dim)
    values = value_cache.reshape(count_seq, cache_len, kv_count, head_dim)
    scale = head_dim ** (-0.5)
    scores = jnp.einsum("bkgd,bjkd->bkgj", query, keys, preferred_element_type=jnp.float32) * scale
    own = (
        jnp.sum(query.astype(jnp.float32) * key_new.astype(jnp.float32)[:, :, None, :], axis=-1)
        * scale
    )
    valid = (lax.broadcasted_iota(jnp.int32, (count_seq, cache_len), 1) < lengths[:, None])[
        :, None, None, :
    ]
    top = jnp.maximum(jnp.max(jnp.where(valid, scores, -1e30), axis=-1), own)
    weights = jnp.where(valid, jnp.exp(scores - top[..., None]), 0.0)
    own_weight = jnp.exp(own - top)
    total = jnp.sum(weights, axis=-1) + own_weight
    probs = (weights / total[..., None]).astype(jnp.bfloat16)
    own_prob = (own_weight / total).astype(jnp.bfloat16)
    mixed = jnp.einsum("bkgj,bjkd->bkgd", probs, values, preferred_element_type=jnp.float32)
    mixed = (
        mixed
        + own_prob.astype(jnp.float32)[..., None] * value_new.astype(jnp.float32)[:, :, None, :]
    )
    return mixed.astype(jnp.bfloat16).reshape(count_seq, -1)


def per_device(
    hidden,
    query_weight,
    key_weight,
    value_weight,
    output_weight,
    gate_weight,
    up_weight,
    down_weight,
    history,
    slot,
    lengths,
    key_cache,
    value_cache,
):
    trainer = (
        query_weight,
        key_weight,
        value_weight,
        output_weight,
        gate_weight,
        up_weight,
        down_weight,
    )
    count = lax.axis_size("fsdp")
    model = query_weight.shape[0]
    rows = model // count
    seqs = hidden.shape[0]
    mine = lengths.shape[0]
    widths = [query_weight.shape[1], key_weight.shape[1], value_weight.shape[1]]
    group = query_weight.shape[1] // key_weight.shape[1]

    first = exchange(pack_rows(count, output_weight))
    packed = pack_columns(count, trainer[:3])

    def block_of(blocks):
        return lambda device: lax.dynamic_index_in_dim(blocks, device, 0, keepdims=False)

    received = {}
    steps = range(1, count)
    bridges = [count // 2, count // 2 + 1, count // 2 - 2]
    received |= shifted(block_of(packed), [step for step in steps if step not in bridges])
    flat = [tensor.T for tensor in trainer]
    flat[3], flat[6] = output_weight, down_weight
    sent = pack_rows(count, down_weight, maxima(flat))
    second = exchange(sent, first)
    ready = after(packed, first)
    received |= shifted(block_of(ready), bridges[:1])
    slice_here = after(hidden.reshape(-1, LANES), first)
    slices = shifted(lambda device: slice_here, range(2, count, 2))
    slices = lax.optimization_barrier((slices, second))[0]
    slices = from_all(slice_here, slices)
    sent = pack_columns(count, (after(up_weight, first),))
    third = exchange(sent, second)
    ready = after(packed, second)
    received |= shifted(block_of(ready), bridges[1:])

    body = tile_rows(down_weight.shape[0], rows)
    heard = second[:, body:].reshape(count, -1)[:, :7].astype(jnp.float32)
    peaks = lax.pmax(jnp.max(heard, axis=0), "tp")
    factors, new_history = scaling(peaks, history, slot)
    whole_hidden = slices.reshape(count, seqs, rows).transpose(1, 0, 2).reshape(seqs, model)
    widened = whole_hidden.astype(jnp.float32)
    inv_rms = lax.rsqrt(jnp.mean(widened * widened, axis=1) + norm_eps)[:, None]
    fresh = jnp.concatenate(
        [
            jnp.dot(
                whole_hidden,
                quantize(trainer[number], factors[number]),
                preferred_element_type=jnp.float32,
            )
            * inv_rms
            / factors[number]
            for number in range(3)
        ],
        axis=1,
    )
    fresh = fresh.reshape(count, mine, -1)
    heard = by_source(
        block_of(fresh)(lax.axis_index("fsdp")), shifted(block_of(fresh), steps)
    )
    sent = pack_columns(count, (after(gate_weight, second),))
    fourth = exchange(sent, third)

    heard = heard.transpose(1, 0, 2)
    query = heard[:, :, : widths[0]].reshape(mine, -1, HEAD_DIM)
    key_new = heard[:, :, widths[0] : widths[0] + widths[1]].reshape(mine, -1, HEAD_DIM)
    value_new = heard[:, :, widths[0] + widths[1] :].reshape(mine, -1, HEAD_DIM)
    query = rotate(query, lengths).astype(jnp.bfloat16).reshape(mine, -1, group, HEAD_DIM)
    key_new = rotate(key_new, lengths).astype(jnp.bfloat16)
    attention_out = attend(
        query, key_new, value_new.astype(jnp.bfloat16), key_cache, value_cache, lengths
    )
    output_rollout = unpack_rows(count, first, output_weight.shape[0], rows, factors, 3)
    down_rollout = unpack_rows(count, second, down_weight.shape[0], rows, factors, 6)
    (gate_rollout,) = unpack_columns(count, fourth, rows, [gate_weight.shape[1]], factors, (4,))
    (up_rollout,) = unpack_columns(count, third, rows, [up_weight.shape[1]], factors, (5,))
    received = lax.optimization_barrier((received, attention_out))[0]
    arrived = by_source(block_of(packed)(lax.axis_index("fsdp")), received)
    query_rollout, key_rollout, value_rollout = unpack_columns(
        count, arrived, rows, widths, factors, (0, 1, 2)
    )
    return (
        attention_out,
        query_rollout,
        key_rollout,
        value_rollout,
        output_rollout,
        gate_rollout,
        up_rollout,
        down_rollout,
        new_history,
    )


def solution(mesh):
    return jax.shard_map(
        per_device,
        mesh=mesh,
        in_specs=(
            P(None, "fsdp"),
            P(None, ("tp", "fsdp")),
            P(None, ("tp", "fsdp")),
            P(None, ("tp", "fsdp")),
            P(("tp", "fsdp"), None),
            P(None, ("tp", "fsdp")),
            P(None, ("tp", "fsdp")),
            P(("tp", "fsdp"), None),
            P(),
            P(),
            P("fsdp"),
            P("fsdp", None, "tp"),
            P("fsdp", None, "tp"),
        ),
        out_specs=(
            P("fsdp", "tp"),
            P("fsdp", "tp"),
            P("fsdp", "tp"),
            P("fsdp", "tp"),
            P("tp", "fsdp"),
            P("fsdp", "tp"),
            P("fsdp", "tp"),
            P("tp", "fsdp"),
            P(),
        ),
        check_vma=False,
    )
```
